32 devices in a mesh: dp: 4 (over y, x), key: 4 (over z), tensor: 2 (over core).
Axes of the slice: x: 2, y: 2, z: 4, core: 2. Of those that a mesh axis runs over, the one named last changes fastest.
Arguments:
- queries: bfloat16 [4096, 8, 2, 256], P(('dp', 'key'), 'tensor'), may hold values from -6 to 6
- sub_keys: bfloat16 [1024, 8, 2, 256], P('key', 'tensor'), may hold values from -6 to 6
- query_weight: bfloat16 [4096, 4096], P(None, 'tensor'), may hold values from -0.09375 to 0.09375
- sub_choice: int32 [4096, 8, 2, 32], P(('dp', 'key'), 'tensor'), may hold values from 0 to 1023, all different within a row
- pair_choice: int32 [4096, 8, 32], P(('dp', 'key'), 'tensor'), may hold values from 0 to 1023, all different within a row
- weights: float32 [4096, 8, 32], P(('dp', 'key'), 'tensor'), may hold values from 0 to 1, as said below
- weight_grad: float32 [4096, 8, 32], P(('dp', 'key'), 'tensor'), may hold values from -6 to 6
Outputs:
- sub_key_grad: float32 [1024, 8, 2, 256], P(('dp', 'key'), 'tensor')
- input_grad: bfloat16 [4096, 4096], P(('dp', 'key', 'tensor'))
The draws below stay inside these ranges and needn't reach their ends.
Inputs may be any that keep to these rules, and one draw needn't show every extreme that they name: Each row of weights is positive and sums to one.
All inputs are finite; a program needn't handle non-finite values.
Results may differ from the reference program's by a relative error of at most 0.0058.
Values may be sent and summed in bfloat16 or wider, within the bound.
No kernel may reach another device: no remote copies, remote signals or barrier semaphores. Data moves between devices by JAX's collectives and lax.ppermute only.
A program may use at most 128 MiB of HBM per device.

```python
import math
import jax
import jax.numpy as jnp
from jax import lax

D = 4096
HEADS = 8
NSUB = 1024
SUBW = 256
TOPK = 32
TOKENS = 4096


def draw_weights(key, part):
    scores = jax.random.normal(key, (TOKENS, HEADS, TOPK), jnp.float32) * 2.0
    return jax.nn.softmax(scores, axis=-1)


def steps_of(key, shape, pieces, low, largest):
    def one(position, blocks):
        heights = jax.random.uniform(jax.random.fold_in(jax.random.fold_in(key, 6), position), (blocks,), jnp.float32, low / len(pieces), largest / len(pieces))
        return jnp.repeat(jnp.exp(heights), shape[position] // blocks).reshape((-1,) + (1,) * (len(shape) - position - 1))

    loudness = one(*pieces[0])
    for cut in pieces[1:]:
        loudness = loudness * one(*cut)
    return loudness


def different_ones(key, rows, amount, top, lift):
    order = jax.random.permutation(jax.random.fold_in(key, 1), amount)
    boost = order
    for power in range(3):
        boost = boost * boost // amount
    boost = boost * lift // amount
    lots = jax.random.randint(jax.random.fold_in(key, 2), (rows, amount), 0, 4096) + boost
    sure = jax.random.permutation(jax.random.fold_in(key, 3), rows)[jnp.arange(amount) % rows]
    lots = jnp.where(jnp.arange(rows)[:, None] == sure[None, :], 1 << 14, lots)
    priority = lots * amount + jnp.arange(amount)
    return lax.top_k(priority.astype(jnp.int32), top)[1].astype(jnp.int32)


def centred(own_key, dims, scale, bound, cuts=(), kind=jnp.bfloat16):
    result = scale * jax.random.normal(own_key, dims, jnp.float32)
    if cuts:
        result = result * steps_of(own_key, dims, cuts, -0.22, 0.18)
    return jnp.clip(result, -bound, bound).astype(kind)


def setup_inputs(seed: int = 0) -> dict:
    key_of = jax.random.split(jax.random.key(seed), 8)
    queries = centred(key_of[0], (TOKENS, HEADS, 2, SUBW), 1.0, 6.0, ((0, 16), (1, 2)))
    sub_keys = centred(key_of[1], (NSUB, HEADS, 2, SUBW), 1.0, 6.0, ((0, 4), (1, 2)))
    query_weight = centred(key_of[2], (D, HEADS * 2 * SUBW), D ** -0.5, 0.09375, ((1, 2),))
    sub_choice = different_ones(key_of[3], TOKENS * HEADS * 2, NSUB, TOPK, 256).reshape((TOKENS, HEADS, 2, TOPK))
    pair_choice = different_ones(key_of[4], TOKENS * HEADS, TOPK * TOPK, TOPK, 0).reshape((TOKENS, HEADS, TOPK))
    weights = draw_weights(jax.random.fold_in(key_of[7], 71), 0)
    weight_grad = centred(key_of[6], (TOKENS, HEADS, TOPK), 1.0, 6.0, ((0, 16), (1, 2)), jnp.float32)
    return dict(queries=queries, sub_keys=sub_keys, query_weight=query_weight, sub_choice=sub_choice, pair_choice=pair_choice, weights=weights, weight_grad=weight_grad)


def row_table(queries_blk, sub_idx, pairs, weights, weight_grad):
    tok = pairs.shape[0]
    score_grad = weights * (weight_grad - jnp.sum(weights * weight_grad, axis=-1, keepdims=True))
    slots = jnp.arange(TOPK, dtype=jnp.int32)
    first = pairs // TOPK
    second = pairs % TOPK
    grad_one = jnp.sum(score_grad[..., None] * (first[..., None] == slots).astype(jnp.float32), axis=2)
    grad_two = jnp.sum(score_grad[..., None] * (second[..., None] == slots).astype(jnp.float32), axis=2)
    slot_grad = jnp.stack([grad_one, grad_two], axis=2)
    count = tok * HEADS * 2
    flat_grad = slot_grad.reshape(count, TOPK)
    flat_idx = sub_idx.reshape(count, TOPK).astype(jnp.int32)
    lines = jnp.arange(count, dtype=jnp.int32)[:, None]
    table = jnp.zeros((count, NSUB), jnp.float32).at[lines, flat_idx].add(flat_grad)
    return table.astype(jnp.bfloat16).reshape(tok, HEADS, 2, NSUB)


def reference(queries, sub_keys, query_weight, sub_choice, pair_choice, weights, weight_grad):
    block = math.gcd(TOKENS, 512)
    nblk = TOKENS // block

    def step(carry, index):
        start = index * block
        q_blk = lax.dynamic_slice_in_dim(queries, start, block, 0)
        s_blk = lax.dynamic_slice_in_dim(sub_choice, start, block, 0)
        p_blk = lax.dynamic_slice_in_dim(pair_choice, start, block, 0)
        w_blk = lax.dynamic_slice_in_dim(weights, start, block, 0)
        g_blk = lax.dynamic_slice_in_dim(weight_grad, start, block, 0)
        table = row_table(q_blk, s_blk, p_blk, w_blk, g_blk)
        query_grad = jnp.einsum("thxr,rhxf->thxf", table.astype(jnp.float32), sub_keys.astype(jnp.float32)).astype(jnp.bfloat16)
        carry = carry + jnp.einsum("thxr,thxf->rhxf", table.astype(jnp.float32), q_blk.astype(jnp.float32))
        flat = query_grad.reshape(block, HEADS * 2 * SUBW)
        out_blk = lax.dot_general(flat, query_weight, (((1,), (1,)), ((), ())), preferred_element_type=jnp.float32)
        return carry, out_blk.astype(jnp.bfloat16)

    start_grad = jnp.zeros((NSUB, HEADS, 2, SUBW), jnp.float32)
    sub_key_grad, blocks = lax.scan(step, start_grad, jnp.arange(nblk, dtype=jnp.int32))
    return sub_key_grad, blocks.reshape(TOKENS, D)
```

```python
import functools
import math

import jax
import jax.numpy as jnp
from jax import lax
from jax.experimental import pallas as pl
from jax.experimental.pallas import tpu as pltpu
from jax.sharding import PartitionSpec as P


F32 = jnp.float32
BF16 = jnp.bfloat16
VMEM_LIMIT = 24 * 1024 * 1024


def whole(memory_space=pltpu.VMEM):
    return pl.BlockSpec(memory_space=memory_space)


def row_code(rows):
    return (((rows & 127) + 128) << (rows >> 7)).astype(F32)


def prep_kernel(groups, per, topk, *refs):
    away, refs = refs[:4], refs[4:]
    outs, refs = refs[:groups], refs[groups:]
    here, sems = refs[:4], refs[4]
    copies = [pltpu.make_async_copy(a, b, sems.at[i]) for i, (a, b) in enumerate(zip(away, here))]
    for copy in copies:
        copy.start()
    for copy in copies:
        copy.wait()
    pair_ref, w_ref, wg_ref, sub_ref = here
    mine = lax.rem(lax.axis_index("dp"), groups)
    tok = pair_ref.shape[-1]
    slots = lax.broadcasted_iota(jnp.int32, (topk, tok), 0)
    for d in range(groups):
        for p in range(per):
            h = (mine ^ d) * per + p
            w = w_ref[h]
            wg = wg_ref[h]
            score = w * (wg - jnp.sum(w * wg, axis=0, keepdims=True))
            pairs = pair_ref[h]
            for x in range(2):
                slot = pairs // topk if x == 0 else pairs % topk
                grad = jnp.zeros((topk, tok), F32)
                for n in range(topk):
                    grad = grad + jnp.where(slot[n : n + 1] == slots, score[n : n + 1], 0.0)
                outs[d][p, x, 0] = row_code(sub_ref[h, x]).astype(BF16)
                outs[d][p, x, 1] = grad.astype(BF16)


def table_kernel(groups, per, topk, *refs):
    tabs, refs = refs[:groups], refs[groups:]
    table, code, value, names = refs
    nsub, wide = table.shape[1:]
    tok = wide // groups
    lanes, tile = 128, 16
    high = math.gcd(512, nsub)
    names[...] = row_code(lax.broadcasted_iota(jnp.int32, (nsub, lanes), 0))
    for p in range(per):
        for x in range(2):
            u = p * 2 + x
            for d in range(groups):
                code[:, d * tok : (d + 1) * tok] = tabs[d][p, x, 0].astype(F32)
                value[:, d * tok : (d + 1) * tok] = tabs[d][p, x, 1].astype(F32)

            def build(b, carry):
                row0 = lax.rem(b, nsub // high) * high
                lane0 = pl.multiple_of(lax.div(b, nsub // high) * lanes, lanes)
                rows = [pl.ds(pl.multiple_of(row0 + m * tile, tile), tile) for m in range(high // tile)]
                name = [names[r, :].astype(BF16) for r in rows]
                acc = [jnp.zeros((tile, lanes), BF16)] * len(rows)
                for s in range(topk):
                    c = jnp.broadcast_to(code[s : s + 1, pl.ds(lane0, lanes)], (tile, lanes)).astype(BF16)
                    v = jnp.broadcast_to(value[s : s + 1, pl.ds(lane0, lanes)], (tile, lanes)).astype(BF16)
                    acc = [jnp.where(n == c, v, a) for n, a in zip(name, acc)]
                for r, a in zip(rows, acc):
                    table[u, r, pl.ds(lane0, lanes)] = a
                return carry

            lax.fori_loop(0, (nsub // high) * (wide // lanes), build, 0)


def mix_kernel(groups, nkey, per, *refs):
    table, refs = refs[0], refs[1:]
    qs, refs = refs[:groups], refs[groups:]
    parts, total = refs[:nkey], refs[nkey]
    k = lax.axis_index("key")
    nsub = table.shape[1]
    tok, width = qs[0].shape[2:]
    blk = total.shape[1]
    high = min(256, nsub)
    for u in range(per * 2):
        for r in range(nsub // high):
            rows = slice(r * high, (r + 1) * high)
            acc = jnp.zeros((high, width), F32)
            for d in range(groups):
                acc = acc + jnp.dot(
                    table[u, rows, d * tok : (d + 1) * tok], qs[d][u // 2, u % 2], preferred_element_type=F32
                )
            per_blk = high // blk
            total[r * per_blk : (r + 1) * per_blk] = acc.reshape(per_blk, blk, width)
        for e in range(nkey):
            for m in range(parts[e].shape[1]):
                parts[e][u, m] = total[m * nkey + (k ^ e)].astype(parts[e].dtype)


def back_kernel(groups, nkey, per, *refs):
    table, refs = refs[0], refs[1:]
    ks, qgs = refs[:nkey], refs[nkey:]
    k = lax.axis_index("key")
    part = ks[0].shape[2]
    width, tok = qgs[0].shape[2:]
    for u in range(per * 2):
        p, x = u // 2, u % 2
        turned = [ks[e][p, x].T for e in range(nkey)]
        for d in range(groups):
            acc = jnp.zeros((width, tok), F32)
            for e in range(nkey):
                off = pl.multiple_of((k ^ e) * part, part)
                acc = acc + jnp.dot(
                    turned[e],
                    table[u, pl.ds(off, part), d * tok : (d + 1) * tok],
                    preferred_element_type=F32,
                )
            qgs[d][p, x] = acc.astype(BF16)


def sum_kernel(groups, nkey, *refs):
    ins, outs = refs[:nkey], refs[nkey:]
    mine = lax.rem(lax.axis_index("dp"), groups)
    for d in range(groups):
        acc = ins[0][:, mine ^ d]
        for e in range(1, nkey):
            acc = acc + ins[e][:, mine ^ d].astype(F32)
        outs[d][...] = acc.astype(outs[d].dtype)


def out_kernel(groups, ntensor, per, *refs):
    qgs, refs = refs[:groups], refs[groups:]
    w_ref, refs = refs[0], refs[1:]
    outs, right = refs[:ntensor], refs[ntensor]
    width, tok = qgs[0].shape[2:]
    here = tok // ntensor

    @pl.when(pl.program_id(0) == 0)
    def _():
        mine = lax.rem(lax.axis_index("dp"), groups)
        for d in range(groups):
            for p in range(per):
                for x in range(2):
                    u = ((mine ^ d) * per + p) * 2 + x
                    right[pl.ds(pl.multiple_of(u * width, width), width), :] = qgs[d][p, x]

    c = lax.axis_index("tensor")
    acc = jnp.dot(w_ref[...], right[...], preferred_element_type=F32)
    pieces = [acc[:, e * here : (e + 1) * here] for e in range(ntensor)]
    for e in range(ntensor):
        piece = pieces[0]
        for j in range(1, ntensor):
            piece = jnp.where((c ^ e) == j, pieces[j], piece)
        outs[e][...] = piece.astype(outs[e].dtype)


def join_kernel(*refs):
    acc = refs[0][...]
    for r in refs[1:-1]:
        acc = acc + r[...].astype(F32)
    refs[-1][...] = acc.T.astype(refs[-1].dtype)


def swap(x, axis, size, d):
    return lax.ppermute(x, axis, [(i, i ^ d) for i in range(size)])


def on_device(queries, sub_keys, query_weight, sub_choice, pair_choice, weights, weight_grad):
    tok, heads, halves, width = queries.shape
    topk = pair_choice.shape[2]
    ndp, nkey, ntensor = (lax.axis_size(a) for a in ("dp", "key", "tensor"))
    part = sub_keys.shape[0]
    nsub = part * nkey
    groups = math.gcd(ndp, heads)
    per = heads // groups
    rest = ndp // groups
    blk = nsub // (ndp * nkey)
    units = per * halves
    mine = lax.rem(lax.axis_index("dp"), groups)
    params = pltpu.CompilerParams(vmem_limit_bytes=VMEM_LIMIT)

    def of_heads(array, first):
        return jnp.transpose(lax.dynamic_slice_in_dim(array, first * per, per, 1), (1, 2, 0, 3))

    raw = (
        jnp.transpose(pair_choice, (1, 2, 0)),
        jnp.transpose(weights, (1, 2, 0)),
        jnp.transpose(weight_grad, (1, 2, 0)),
        jnp.transpose(sub_choice, (1, 2, 3, 0)),
    )
    tabs = pl.pallas_call(
        functools.partial(prep_kernel, groups, per, topk),
        out_shape=[jax.ShapeDtypeStruct((per, halves, 2, topk, tok), BF16)] * groups,
        in_specs=[whole(pltpu.HBM)] * 4,
        out_specs=[whole()] * groups,
        scratch_shapes=[pltpu.VMEM(r.shape, r.dtype) for r in raw] + [pltpu.SemaphoreType.DMA((4,))],
        compiler_params=params,
        name="prep",
    )(*[pltpu.with_memory_space_constraint(r, pltpu.HBM) for r in raw])
    own_keys = of_heads(sub_keys, mine)
    keys = [own_keys] + [swap(own_keys, "key", nkey, e) for e in range(1, nkey)]
    tabs = [tabs[0]] + [swap(tabs[d], "dp", ndp, d) for d in range(1, groups)]
    qs = [of_heads(queries, mine ^ d) for d in range(groups)]
    qs = [qs[0]] + [swap(qs[d], "dp", ndp, d) for d in range(1, groups)]

    table = pl.pallas_call(
        functools.partial(table_kernel, groups, per, topk),
        out_shape=jax.ShapeDtypeStruct((units, nsub, groups * tok), BF16),
        in_specs=[whole()] * groups,
        out_specs=whole(),
        scratch_shapes=[
            pltpu.VMEM((topk, groups * tok), F32),
            pltpu.VMEM((topk, groups * tok), F32),
            pltpu.VMEM((nsub, 128), F32),
        ],
        compiler_params=params,
        name="table",
    )(*tabs)
    parts = pl.pallas_call(
        functools.partial(mix_kernel, groups, nkey, per),
        out_shape=[
            jax.ShapeDtypeStruct((units, ndp, blk, width), F32 if e == 0 else BF16) for e in range(nkey)
        ],
        in_specs=[whole()] * (1 + groups),
        out_specs=[whole()] * nkey,
        scratch_shapes=[pltpu.VMEM((ndp * nkey, blk, width), F32)],
        compiler_params=params,
        name="mix",
    )(table, *qs)
    qgs = pl.pallas_call(
        functools.partial(back_kernel, groups, nkey, per),
        out_shape=[jax.ShapeDtypeStruct((per, halves, width, tok), BF16)] * groups,
        in_specs=[whole()] * (1 + nkey),
        out_specs=[whole()] * groups,
        compiler_params=params,
        name="back",
    )(table, *keys)
    parts = [parts[0]] + [swap(parts[e], "key", nkey, e) for e in range(1, nkey)]
    qgs = [qgs[0]] + [swap(qgs[d], "dp", ndp, d) for d in range(1, groups)]

    if rest > 1:
        summed = parts[0]
        for e in range(1, nkey):
            summed = summed + parts[e].astype(F32)
        summed = lax.psum_scatter(
            summed.reshape(units, rest, groups, blk, width),
            "dp",
            scatter_dimension=1,
            axis_index_groups=[[r * groups + g for r in range(rest)] for g in range(groups)],
            tiled=True,
        ).reshape(units, groups, blk, width)
        parts = [summed]
    pieces = pl.pallas_call(
        functools.partial(sum_kernel, groups, len(parts)),
        out_shape=[jax.ShapeDtypeStruct((units, blk, width), F32 if d == 0 else BF16) for d in range(groups)],
        in_specs=[whole()] * len(parts),
        out_specs=[whole()] * groups,
        compiler_params=params,
        name="sum",
    )(*parts)
    pieces = [pieces[0]] + [swap(pieces[d], "dp", ndp, d).astype(F32) for d in range(1, groups)]
    stacked = jnp.stack(pieces).reshape(groups, per, halves, blk, width)
    order = jnp.stack([lax.dynamic_index_in_dim(stacked, mine ^ d, 0, False) for d in range(groups)])
    sub_key_grad = jnp.transpose(order, (3, 0, 1, 2, 4)).reshape(blk, heads, halves, width)

    rows = query_weight.shape[0]
    bn = math.gcd(rows, 512)
    here = tok // ntensor
    outs = pl.pallas_call(
        functools.partial(out_kernel, groups, ntensor, per),
        out_shape=[jax.ShapeDtypeStruct((rows, here), F32 if e == 0 else BF16) for e in range(ntensor)],
        grid=(rows // bn,),
        in_specs=[pl.BlockSpec((per, halves, width, tok), lambda i: (0, 0, 0, 0))] * groups
        + [pl.BlockSpec((bn, heads * halves * width), lambda i: (i, 0))],
        out_specs=[pl.BlockSpec((bn, here), lambda i: (i, 0))] * ntensor,
        scratch_shapes=[pltpu.VMEM((heads * halves * width, tok), BF16)],
        compiler_params=params,
        name="out",
    )(*qgs, query_weight)
    outs = [outs[0]] + [swap(outs[e], "tensor", ntensor, e) for e in range(1, ntensor)]
    input_grad = pl.pallas_call(
        join_kernel,
        out_shape=jax.ShapeDtypeStruct((here, rows), BF16),
        in_specs=[whole()] * ntensor,
        out_specs=whole(),
        compiler_params=params,
        name="join",
    )(*outs)
    return sub_key_grad, input_grad


def solution(mesh):
    in_specs = (
        P(("dp", "key"), "tensor", None, None),
        P("key", "tensor", None, None),
        P(None, "tensor"),
        P(("dp", "key"), "tensor", None, None),
        P(("dp", "key"), "tensor", None),
        P(("dp", "key"), "tensor", None),
        P(("dp", "key"), "tensor", None),
    )
    out_specs = (P(("dp", "key"), "tensor", None, None), P(("dp", "key", "tensor"), None))

    return jax.shard_map(on_device, mesh=mesh, in_specs=in_specs, out_specs=out_specs, check_vma=False)
```

```python
import functools
import math

import jax
import jax.numpy as jnp
from jax import lax
from jax.experimental import pallas as pl
from jax.experimental.pallas import tpu as pltpu
from jax.sharding import PartitionSpec as P


F32 = jnp.float32
BF16 = jnp.bfloat16
VMEM_LIMIT = 12 * 1024 * 1024


def whole(memory_space=pltpu.VMEM):
    return pl.BlockSpec(memory_space=memory_space)


def row_code(rows):
    return (((rows & 127) + 128) << (rows >> 7)).astype(F32)


def prep_kernel(groups, per, topk, *refs):
    away, refs = refs[:4], refs[4:]
    outs, refs = refs[:groups], refs[groups:]
    here, sems = refs[:4], refs[4]
    copies = [pltpu.make_async_copy(a, b, sems.at[i]) for i, (a, b) in enumerate(zip(away, here))]
    for copy in copies:
        copy.start()
    for copy in copies:
        copy.wait()
    pair_ref, w_ref, wg_ref, sub_ref = here
    mine = lax.rem(lax.axis_index("dp"), groups)
    tok = pair_ref.shape[-1]
    slots = lax.broadcasted_iota(jnp.int32, (topk, tok), 0)
    for d in range(groups):
        for p in range(per):
            h = (mine ^ d) * per + p
            w = w_ref[h]
            wg = wg_ref[h]
            score = w * (wg - jnp.sum(w * wg, axis=0, keepdims=True))
            pairs = pair_ref[h]
            for x in range(2):
                slot = pairs // topk if x == 0 else pairs % topk
                grad = jnp.zeros((topk, tok), F32)
                for n in range(topk):
                    grad = grad + jnp.where(slot[n : n + 1] == slots, score[n : n + 1], 0.0)
                outs[d][p, x, 0] = row_code(sub_ref[h, x]).astype(BF16)
                outs[d][p, x, 1] = grad.astype(BF16)


def table_kernel(units, topk, n, *refs):
    tabs, refs = refs[:n], refs[n:]
    tables, (code, value, names) = refs[: len(units)], refs[len(units) :]
    nsub, wide = tables[0].shape
    tok = wide // n
    lanes, tile = 128, 16
    high = math.gcd(512, nsub)
    names[...] = row_code(lax.broadcasted_iota(jnp.int32, (nsub, lanes), 0))
    for table, u in zip(tables, units):
        for d in range(n):
            code[:, d * tok : (d + 1) * tok] = tabs[d][u // 2, u % 2, 0].astype(F32)
            value[:, d * tok : (d + 1) * tok] = tabs[d][u // 2, u % 2, 1].astype(F32)

        def build(b, carry, table=table):
            row0 = lax.rem(b, nsub // high) * high
            lane0 = pl.multiple_of(lax.div(b, nsub // high) * lanes, lanes)
            rows = [pl.ds(pl.multiple_of(row0 + m * tile, tile), tile) for m in range(high // tile)]
            name = [names[r, :].astype(BF16) for r in rows]
            acc = [jnp.zeros((tile, lanes), BF16)] * len(rows)
            for s in range(topk):
                c = jnp.broadcast_to(code[s : s + 1, pl.ds(lane0, lanes)], (tile, lanes)).astype(BF16)
                v = jnp.broadcast_to(value[s : s + 1, pl.ds(lane0, lanes)], (tile, lanes)).astype(BF16)
                acc = [jnp.where(n == c, v, a) for n, a in zip(name, acc)]
            for r, a in zip(rows, acc):
                table[r, pl.ds(lane0, lanes)] = a
            return carry

        lax.fori_loop(0, (nsub // high) * (wide // lanes), build, 0)


def columns(d, tok):
    return slice(max(d - 1, 0) * tok, max(d - 1, 0) * tok + tok)


def mix_kernel(groups, keep_of, send_of, p, x, *refs):
    tables, refs = refs[: min(groups, 2)], refs[min(groups, 2) :]
    qs, refs = refs[:groups], refs[groups:]
    keep, send, total = refs
    k = lax.axis_index("key")
    nkey = len(keep_of) + len(send_of)
    nsub = tables[0].shape[0]
    tok, width = qs[0].shape[2:]
    blk = total.shape[1]
    high = min(256, nsub)
    for r in range(nsub // high):
        rows = slice(r * high, (r + 1) * high)
        acc = jnp.zeros((high, width), F32)
        for d in range(groups):
            acc = acc + jnp.dot(
                tables[min(d, 1)][rows, columns(d, tok)], qs[d][p, x], preferred_element_type=F32
            )
        per_blk = high // blk
        total[r * per_blk : (r + 1) * per_blk] = acc.reshape(per_blk, blk, width)
    for ref, which in ((keep, keep_of), (send, send_of)):
        for i, e in enumerate(which):
            for m in range(ref.shape[1]):
                ref[i, m] = total[m * nkey + (k ^ e)].astype(ref.dtype)


def halve_kernel(keep_at, send_at, kept, got, keep, send):
    for ref, which in ((keep, keep_at), (send, send_at)):
        for i, at in enumerate(which):
            ref[i] = (kept[at] + got[at].astype(F32)).astype(ref.dtype)


def back_kernel(groups, nkey, per, *refs):
    units = per * 2
    both = min(groups, 2)
    tables, refs = refs[: units * both], refs[units * both :]
    ks, qgs = refs[:nkey], refs[nkey:]
    k = lax.axis_index("key")
    part = ks[0].shape[2]
    width, tok = qgs[0].shape[2:]
    for u in range(units):
        p, x = u // 2, u % 2
        turned = [ks[e][p, x].T for e in range(nkey)]
        for d in range(groups):
            acc = jnp.zeros((width, tok), F32)
            for e in range(nkey):
                off = pl.multiple_of((k ^ e) * part, part)
                acc = acc + jnp.dot(
                    turned[e],
                    tables[u * both + min(d, 1)][pl.ds(off, part), columns(d, tok)],
                    preferred_element_type=F32,
                )
            qgs[d][p, x] = acc.astype(BF16)


def sum_kernel(groups, units, *refs):
    ins, outs = refs[:-groups], refs[-groups:]
    mine = lax.rem(lax.axis_index("dp"), groups)
    each = len(ins) // units
    for u in range(units):
        for d in range(groups):
            acc = ins[u * each][mine ^ d]
            for r in ins[u * each + 1 : (u + 1) * each]:
                acc = acc + r[mine ^ d].astype(F32)
            outs[d][u] = acc.astype(outs[d].dtype)


def first_kernel(groups, ds, per, *refs):
    qgs, (w_ref, out, right) = refs[: len(ds)], refs[len(ds) :]
    multiply(groups, ds, per, qgs, w_ref, right, out, None)


def second_kernel(groups, ds, ntensor, per, *refs):
    qgs, refs = refs[: len(ds)], refs[len(ds) :]
    w_ref, begun, refs = refs[0], refs[1], refs[2:]
    outs, right = refs[:ntensor], refs[ntensor]
    multiply(groups, ds, per, qgs, w_ref, right, outs, begun)


def multiply(groups, ds, per, qgs, w_ref, right, outs, begun):
    mine = lax.rem(lax.axis_index("dp"), groups)
    width, tok = qgs[0].shape[2:]
    span = per * 2 * width
    for i in range(len(ds)):
        for u in range(per * 2):
            right[i * span + u * width : i * span + (u + 1) * width, :] = qgs[i][u // 2, u % 2]
    offs = [pl.multiple_of((mine ^ d) * span, span) for d in ds]
    rows = w_ref.shape[0]
    high = math.gcd(rows, 512)

    def body(b, carry):
        at = pl.ds(pl.multiple_of(b * high, high), high)
        acc = jnp.zeros((high, tok), F32) if begun is None else begun[at, :]
        for i, off in enumerate(offs):
            acc = acc + jnp.dot(
                w_ref[at, pl.ds(off, span)], right[i * span : (i + 1) * span, :], preferred_element_type=F32
            )
        if begun is None:
            outs[at, :] = acc
            return carry
        n = len(outs)
        here = tok // n
        c = lax.axis_index("tensor")
        pieces = [acc[:, e * here : (e + 1) * here] for e in range(n)]
        for e in range(n):
            piece = pieces[0]
            for j in range(1, n):
                piece = jnp.where((c ^ e) == j, pieces[j], piece)
            outs[e][at, :] = piece.astype(outs[e].dtype)
        return carry

    lax.fori_loop(0, rows // high, body, 0)


def join_kernel(*refs):
    acc = refs[0][...]
    for r in refs[1:-1]:
        acc = acc + r[...].astype(F32)
    refs[-1][...] = acc.T.astype(refs[-1].dtype)


def swap(x, axis, size, d):
    return lax.ppermute(x, axis, [(i, i ^ d) for i in range(size)])


def on_device(queries, sub_keys, query_weight, sub_choice, pair_choice, weights, weight_grad):
    tok, heads, halves, width = queries.shape
    topk = pair_choice.shape[2]
    ndp, nkey, ntensor = (lax.axis_size(a) for a in ("dp", "key", "tensor"))
    part = sub_keys.shape[0]
    nsub = part * nkey
    groups = math.gcd(ndp, heads)
    per = heads // groups
    rest = ndp // groups
    blk = nsub // (ndp * nkey)
    units = per * halves
    mine = lax.rem(lax.axis_index("dp"), groups)
    params = pltpu.CompilerParams(vmem_limit_bytes=VMEM_LIMIT)

    def of_heads(array, first):
        return jnp.transpose(lax.dynamic_slice_in_dim(array, first * per, per, 1), (1, 2, 0, 3))

    raw = (
        jnp.transpose(pair_choice, (1, 2, 0)),
        jnp.transpose(weights, (1, 2, 0)),
        jnp.transpose(weight_grad, (1, 2, 0)),
        jnp.transpose(sub_choice, (1, 2, 3, 0)),
    )
    tabs = pl.pallas_call(
        functools.partial(prep_kernel, groups, per, topk),
        out_shape=[jax.ShapeDtypeStruct((per, halves, 2, topk, tok), BF16)] * groups,
        in_specs=[whole(pltpu.HBM)] * 4,
        out_specs=[whole()] * groups,
        scratch_shapes=[pltpu.VMEM(r.shape, r.dtype) for r in raw] + [pltpu.SemaphoreType.DMA((4,))],
        compiler_params=params,
        name="prep",
    )(*[pltpu.with_memory_space_constraint(r, pltpu.HBM) for r in raw])
    own_keys = of_heads(sub_keys, mine)
    keys = [own_keys] + [swap(own_keys, "key", nkey, e) for e in range(1, nkey)]
    tabs = [tabs[0]] + [swap(tabs[d], "dp", ndp, d) for d in range(1, groups)]
    qs = [of_heads(queries, mine ^ d) for d in range(groups)]
    qs = [qs[0]] + [swap(qs[d], "dp", ndp, d) for d in range(1, groups)]

    def call(kernel, outs, *ins, scratch=()):
        many = isinstance(outs, (list, tuple))
        return pl.pallas_call(
            kernel,
            out_shape=outs,
            in_specs=[whole()] * len(ins),
            out_specs=[whole()] * len(outs) if many else whole(),
            scratch_shapes=list(scratch),
            compiler_params=params,
        )(*ins)

    shape = jax.ShapeDtypeStruct
    left = list(range(nkey))
    keep_of = [e for e in left if not e & 1]
    send_of = [e for e in left if e & 1]
    tables, halves_of = [], []

    def build(which, sources):
        wide = len(sources) * tok
        return call(
            functools.partial(table_kernel, which, topk, len(sources)),
            [shape((nsub, wide), BF16)] * len(which),
            *sources,
            scratch=[
                pltpu.VMEM((topk, wide), F32),
                pltpu.VMEM((topk, wide), F32),
                pltpu.VMEM((nsub, 128), F32),
            ],
        )

    mine_tables = build(list(range(units)), tabs[:1])
    tabs = tabs[1:]
    for u in range(units):
        p, x = u // halves, u % halves
        table = [mine_tables[u]] + (list(build([u], tabs)) if tabs else [])
        keep, send = call(
            functools.partial(mix_kernel, groups, keep_of, send_of, p, x),
            [
                shape((len(keep_of), ndp, blk, width), F32),
                shape((len(send_of), ndp, blk, width), BF16),
            ],
            *table,
            *qs,
            scratch=[pltpu.VMEM((ndp * nkey, blk, width), F32)],
        )
        got = swap(send, "key", nkey, 1)
        tables += table
        halves_of.append((keep, got))
    qgs = call(
        functools.partial(back_kernel, groups, nkey, per),
        [shape((per, halves, width, tok), BF16)] * groups,
        *tables,
        *keys,
    )
    qgs = [qgs[0]] + [swap(qgs[d], "dp", ndp, d) for d in range(1, groups)]

    parts = []
    for keep, got in halves_of:
        left, bit = keep_of, 2
        while len(left) > 1:
            keep_at = [i for i, e in enumerate(left) if not e & bit]
            send_at = [i for i, e in enumerate(left) if e & bit]
            keep, send = call(
                functools.partial(halve_kernel, keep_at, send_at),
                [
                    shape((len(keep_at), ndp, blk, width), F32),
                    shape((len(send_at), ndp, blk, width), BF16),
                ],
                keep,
                got,
            )
            got = swap(send, "key", nkey, bit)
            left, bit = [left[i] for i in keep_at], bit * 2
        parts += [keep.reshape(ndp, blk, width), got.reshape(ndp, blk, width)]

    if rest > 1:
        summed = jnp.stack([parts[2 * u] + parts[2 * u + 1].astype(F32) for u in range(units)])
        summed = lax.psum_scatter(
            summed.reshape(units, rest, groups, blk, width),
            "dp",
            scatter_dimension=1,
            axis_index_groups=[[r * groups + g for r in range(rest)] for g in range(groups)],
            tiled=True,
        ).reshape(units, groups, blk, width)
        parts = [summed[u] for u in range(units)]
    pieces = call(
        functools.partial(sum_kernel, groups, units),
        [shape((units, blk, width), F32 if d == 0 else BF16) for d in range(groups)],
        *parts,
    )
    pieces = [pieces[0]] + [swap(pieces[d], "dp", ndp, d) for d in range(1, groups)]
    pieces = [p.astype(F32) for p in pieces]
    stacked = jnp.stack(pieces).reshape(groups, per, halves, blk, width)
    order = jnp.stack([lax.dynamic_index_in_dim(stacked, mine ^ d, 0, False) for d in range(groups)])
    sub_key_grad = jnp.transpose(order, (3, 0, 1, 2, 4)).reshape(blk, heads, halves, width)

    rows = query_weight.shape[0]
    here = tok // ntensor
    early = [0] if groups > 1 else []
    late = list(range(len(early), groups))
    span = per * halves * width
    if early:
        begun = call(
            functools.partial(first_kernel, groups, early, per),
            shape((rows, tok), F32),
            *[qgs[d] for d in early],
            query_weight,
            scratch=[pltpu.VMEM((len(early) * span, tok), BF16)],
        )
    else:
        begun = jnp.zeros((rows, tok), F32)
    outs = call(
        functools.partial(second_kernel, groups, late, ntensor, per),
        [shape((rows, here), F32 if e == 0 else BF16) for e in range(ntensor)],
        *[qgs[d] for d in late],
        query_weight,
        begun,
        scratch=[pltpu.VMEM((len(late) * span, tok), BF16)],
    )
    outs = [outs[0]] + [swap(outs[e], "tensor", ntensor, e) for e in range(1, ntensor)]
    input_grad = pl.pallas_call(
        join_kernel,
        out_shape=jax.ShapeDtypeStruct((here, rows), BF16),
        in_specs=[whole()] * ntensor,
        out_specs=whole(),
        compiler_params=params,
        name="join",
    )(*outs)
    return sub_key_grad, input_grad


def solution(mesh):
    in_specs = (
        P(("dp", "key"), "tensor", None, None),
        P("key", "tensor", None, None),
        P(None, "tensor"),
        P(("dp", "key"), "tensor", None, None),
        P(("dp", "key"), "tensor", None),
        P(("dp", "key"), "tensor", None),
        P(("dp", "key"), "tensor", None),
    )
    out_specs = (P(("dp", "key"), "tensor", None, None), P(("dp", "key", "tensor"), None))

    return jax.shard_map(
        on_device, mesh=mesh, in_specs=in_specs, out_specs=out_specs, check_vma=False
    )
```

```python
import functools
import math

import jax
import jax.numpy as jnp
from jax import lax
from jax.experimental import pallas as pl
from jax.experimental.pallas import tpu as pltpu
from jax.sharding import PartitionSpec as P


F32 = jnp.float32
BF16 = jnp.bfloat16
VMEM_LIMIT = 12 * 1024 * 1024


def whole(memory_space=pltpu.VMEM):
    return pl.BlockSpec(memory_space=memory_space)


def row_code(rows):
    return (((rows & 127) + 128) << (rows >> 7)).astype(F32)


def prep_kernel(groups, per, topk, *refs):
    away, (q_ref, k_ref), refs = refs[:4], refs[4:6], refs[6:]
    outs, cuts, refs = refs[:groups], refs[groups : 2 * groups + 1], refs[2 * groups + 1 :]
    here, sems = refs[:4], refs[4]
    mine = lax.rem(lax.axis_index("dp"), groups)
    copies = [pltpu.make_async_copy(a, b, sems.at[i]) for i, (a, b) in enumerate(zip(away, here))]
    later = [
        pltpu.make_async_copy(k_ref.at[:, pl.ds(mine * per, per)], cuts[groups], sems.at[4])
    ] + [
        pltpu.make_async_copy(q_ref.at[:, pl.ds((mine ^ d) * per, per)], cuts[d], sems.at[5 + d])
        for d in range(groups)
    ]
    for copy in copies + later:
        copy.start()
    for copy in copies:
        copy.wait()
    pair_ref, w_ref, wg_ref, sub_ref = here
    tok = pair_ref.shape[-1]
    slots = lax.broadcasted_iota(jnp.int32, (topk, tok), 0)
    for d in range(groups):
        for p in range(per):
            h = (mine ^ d) * per + p
            w = w_ref[h]
            wg = wg_ref[h]
            score = w * (wg - jnp.sum(w * wg, axis=0, keepdims=True))
            pairs = pair_ref[h]
            for x in range(2):
                slot = pairs // topk if x == 0 else pairs % topk
                grad = jnp.zeros((topk, tok), F32)
                for n in range(topk):
                    grad = grad + jnp.where(slot[n : n + 1] == slots, score[n : n + 1], 0.0)
                outs[d][p, x, 0] = row_code(sub_ref[h, x]).astype(BF16)
                outs[d][p, x, 1] = grad.astype(BF16)
    for copy in later:
        copy.wait()


def table_kernel(units, topk, n, *refs):
    tabs, refs = refs[:n], refs[n:]
    tables, (code, value, names) = refs[: len(units)], refs[len(units) :]
    nsub, wide = tables[0].shape
    tok = wide // n
    lanes, tile = 128, 16
    high = math.gcd(1024, nsub)
    names[...] = row_code(lax.broadcasted_iota(jnp.int32, (nsub, lanes), 0))
    for table, u in zip(tables, units):
        for d in range(n):
            code[:, d * tok : (d + 1) * tok] = tabs[d][u // 2, u % 2, 0].astype(F32)
            value[:, d * tok : (d + 1) * tok] = tabs[d][u // 2, u % 2, 1].astype(F32)

        def build(b, carry, table=table):
            row0 = lax.rem(b, nsub // high) * high
            lane0 = pl.multiple_of(lax.div(b, nsub // high) * lanes, lanes)
            rows = [pl.ds(pl.multiple_of(row0 + m * tile, tile), tile) for m in range(high // tile)]
            name = [names[r, :].astype(BF16) for r in rows]
            acc = [jnp.zeros((tile, lanes), BF16)] * len(rows)
            for s in range(topk):
                c = jnp.broadcast_to(code[s : s + 1, pl.ds(lane0, lanes)], (tile, lanes)).astype(BF16)
                v = jnp.broadcast_to(value[s : s + 1, pl.ds(lane0, lanes)], (tile, lanes)).astype(BF16)
                acc = [jnp.where(n == c, v, a) for n, a in zip(name, acc)]
            for r, a in zip(rows, acc):
                table[r, pl.ds(lane0, lanes)] = a
            return carry

        lax.fori_loop(0, (nsub // high) * (wide // lanes), build, 0)


def columns(d, tok):
    return slice(max(d - 1, 0) * tok, max(d - 1, 0) * tok + tok)


def mix_kernel(groups, keep_of, send_of, p, x, *refs):
    tables, refs = refs[: min(groups, 2)], refs[min(groups, 2) :]
    qs, refs = refs[:groups], refs[groups:]
    keep, send, total = refs
    k = lax.axis_index("key")
    nkey = len(keep_of) + len(send_of)
    nsub = tables[0].shape[0]
    tok, width = qs[0].shape[2:]
    blk = total.shape[1]
    high = min(256, nsub)
    for r in range(nsub // high):
        rows = slice(r * high, (r + 1) * high)
        acc = jnp.zeros((high, width), F32)
        for d in range(groups):
            acc = acc + jnp.dot(
                tables[min(d, 1)][rows, columns(d, tok)], qs[d][p, x], preferred_element_type=F32
            )
        per_blk = high // blk
        total[r * per_blk : (r + 1) * per_blk] = acc.reshape(per_blk, blk, width)
    for ref, which in ((keep, keep_of), (send, send_of)):
        for i, e in enumerate(which):
            for m in range(ref.shape[1]):
                ref[i, m] = total[m * nkey + (k ^ e)].astype(ref.dtype)


def halve_kernel(keep_at, send_at, kept, got, keep, send):
    for ref, which in ((keep, keep_at), (send, send_at)):
        for i, at in enumerate(which):
            ref[i] = (kept[at] + got[at].astype(F32)).astype(ref.dtype)


def back_kernel(groups, nkey, per, *refs):
    units = per * 2
    both = min(groups, 2)
    tables, refs = refs[: units * both], refs[units * both :]
    ks, qgs = refs[:nkey], refs[nkey:]
    k = lax.axis_index("key")
    part = ks[0].shape[2]
    width, tok = qgs[0].shape[2:]
    for u in range(units):
        p, x = u // 2, u % 2
        turned = [ks[e][p, x].T for e in range(nkey)]
        for d in range(groups):
            acc = jnp.zeros((width, tok), F32)
            for e in range(nkey):
                off = pl.multiple_of((k ^ e) * part, part)
                acc = acc + jnp.dot(
                    turned[e],
                    tables[u * both + min(d, 1)][pl.ds(off, part), columns(d, tok)],
                    preferred_element_type=F32,
                )
            qgs[d][p, x] = acc.astype(BF16)


def sum_kernel(groups, units, *refs):
    ins, outs = refs[:-groups], refs[-groups:]
    mine = lax.rem(lax.axis_index("dp"), groups)
    each = len(ins) // units
    for u in range(units):
        for d in range(groups):
            acc = ins[u * each][mine ^ d]
            for r in ins[u * each + 1 : (u + 1) * each]:
                acc = acc + r[mine ^ d].astype(F32)
            outs[d][u] = acc.astype(outs[d].dtype)


def first_kernel(groups, ds, per, *refs):
    qgs, (w_ref, out, right) = refs[: len(ds)], refs[len(ds) :]
    multiply(groups, ds, per, qgs, w_ref, right, out, None)


def second_kernel(groups, ds, ntensor, per, *refs):
    qgs, refs = refs[: len(ds)], refs[len(ds) :]
    w_ref, begun, refs = refs[0], refs[1], refs[2:]
    outs, right = refs[:ntensor], refs[ntensor]
    multiply(groups, ds, per, qgs, w_ref, right, outs, begun)


def multiply(groups, ds, per, qgs, w_ref, right, outs, begun):
    mine = lax.rem(lax.axis_index("dp"), groups)
    width, tok = qgs[0].shape[2:]
    span = per * 2 * width
    for i in range(len(ds)):
        for u in range(per * 2):
            right[i * span + u * width : i * span + (u + 1) * width, :] = qgs[i][u // 2, u % 2]
    offs = [pl.multiple_of((mine ^ d) * span, span) for d in ds]
    rows = w_ref.shape[0]
    high = math.gcd(rows, 1024)

    for b in range(rows // high):
        at = slice(b * high, (b + 1) * high)
        acc = jnp.zeros((high, tok), F32) if begun is None else begun[at, :]
        for i, off in enumerate(offs):
            acc = acc + jnp.dot(
                w_ref[at, pl.ds(off, span)], right[i * span : (i + 1) * span, :], preferred_element_type=F32
            )
        if begun is None:
            outs[at, :] = acc
            continue
        n = len(outs)
        here = tok // n
        c = lax.axis_index("tensor")
        pieces = [acc[:, e * here : (e + 1) * here] for e in range(n)]
        for e in range(n):
            piece = pieces[0]
            for j in range(1, n):
                piece = jnp.where((c ^ e) == j, pieces[j], piece)
            outs[e][at, :] = piece.astype(outs[e].dtype)


def join_kernel(*refs):
    acc = refs[0][...]
    for r in refs[1:-1]:
        acc = acc + r[...].astype(F32)
    refs[-1][...] = acc.T.astype(refs[-1].dtype)


def swap(x, axis, size, d):
    return lax.ppermute(x, axis, [(i, i ^ d) for i in range(size)])


def on_device(queries, sub_keys, query_weight, sub_choice, pair_choice, weights, weight_grad):
    tok, heads, halves, width = queries.shape
    topk = pair_choice.shape[2]
    ndp, nkey, ntensor = (lax.axis_size(a) for a in ("dp", "key", "tensor"))
    part = sub_keys.shape[0]
    nsub = part * nkey
    groups = math.gcd(ndp, heads)
    per = heads // groups
    rest = ndp // groups
    blk = nsub // (ndp * nkey)
    units = per * halves
    mine = lax.rem(lax.axis_index("dp"), groups)
    params = pltpu.CompilerParams(vmem_limit_bytes=VMEM_LIMIT)

    def by_head(cut):
        return jnp.transpose(cut, (1, 2, 0, 3))

    raw = (
        jnp.transpose(pair_choice, (1, 2, 0)),
        jnp.transpose(weights, (1, 2, 0)),
        jnp.transpose(weight_grad, (1, 2, 0)),
        jnp.transpose(sub_choice, (1, 2, 3, 0)),
    )
    prepared = pl.pallas_call(
        functools.partial(prep_kernel, groups, per, topk),
        out_shape=[jax.ShapeDtypeStruct((per, halves, 2, topk, tok), BF16)] * groups
        + [jax.ShapeDtypeStruct((tok, per, halves, width), BF16)] * groups
        + [jax.ShapeDtypeStruct((part, per, halves, width), BF16)],
        in_specs=[whole(pltpu.HBM)] * 6,
        out_specs=[whole()] * (2 * groups + 1),
        scratch_shapes=[pltpu.VMEM(r.shape, r.dtype) for r in raw]
        + [pltpu.SemaphoreType.DMA((5 + groups,))],
        compiler_params=params,
        name="prep",
    )(*[pltpu.with_memory_space_constraint(r, pltpu.HBM) for r in (*raw, queries, sub_keys)])
    tabs, cuts, own_keys = prepared[:groups], prepared[groups:-1], by_head(prepared[-1])
    keys = [own_keys] + [swap(own_keys, "key", nkey, e) for e in range(1, nkey)]
    tabs = [tabs[0]] + [swap(tabs[d], "dp", ndp, d) for d in range(1, groups)]
    qs = [by_head(cut) for cut in cuts]
    qs = [qs[0]] + [swap(qs[d], "dp", ndp, d) for d in range(1, groups)]

    def call(kernel, outs, *ins, scratch=()):
        many = isinstance(outs, (list, tuple))
        return pl.pallas_call(
            kernel,
            out_shape=outs,
            in_specs=[whole()] * len(ins),
            out_specs=[whole()] * len(outs) if many else whole(),
            scratch_shapes=list(scratch),
            compiler_params=params,
        )(*ins)

    shape = jax.ShapeDtypeStruct
    left = list(range(nkey))
    keep_of = [e for e in left if not e & 1]
    send_of = [e for e in left if e & 1]
    tables, halves_of = [], []

    def build(which, sources):
        wide = len(sources) * tok
        return call(
            functools.partial(table_kernel, which, topk, len(sources)),
            [shape((nsub, wide), BF16)] * len(which),
            *sources,
            scratch=[
                pltpu.VMEM((topk, wide), F32),
                pltpu.VMEM((topk, wide), F32),
                pltpu.VMEM((nsub, 128), F32),
            ],
        )

    mine_tables = build(list(range(units)), tabs[:1])
    tabs = tabs[1:]
    for u in range(units):
        p, x = u // halves, u % halves
        table = [mine_tables[u]] + (list(build([u], tabs)) if tabs else [])
        keep, send = call(
            functools.partial(mix_kernel, groups, keep_of, send_of, p, x),
            [
                shape((len(keep_of), ndp, blk, width), F32),
                shape((len(send_of), ndp, blk, width), BF16),
            ],
            *table,
            *qs,
            scratch=[pltpu.VMEM((ndp * nkey, blk, width), F32)],
        )
        got = swap(send, "key", nkey, 1)
        tables += table
        halves_of.append((keep, got))
    qgs = call(
        functools.partial(back_kernel, groups, nkey, per),
        [shape((per, halves, width, tok), BF16)] * groups,
        *tables,
        *keys,
    )
    qgs = [qgs[0]] + [swap(qgs[d], "dp", ndp, d) for d in range(1, groups)]

    parts = []
    for keep, got in halves_of:
        left, bit = keep_of, 2
        while len(left) > 1:
            keep_at = [i for i, e in enumerate(left) if not e & bit]
            send_at = [i for i, e in enumerate(left) if e & bit]
            keep, send = call(
                functools.partial(halve_kernel, keep_at, send_at),
                [
                    shape((len(keep_at), ndp, blk, width), F32),
                    shape((len(send_at), ndp, blk, width), BF16),
                ],
                keep,
                got,
            )
            got = swap(send, "key", nkey, bit)
            left, bit = [left[i] for i in keep_at], bit * 2
        parts += [keep.reshape(ndp, blk, width), got.reshape(ndp, blk, width)]

    if rest > 1:
        summed = jnp.stack([parts[2 * u] + parts[2 * u + 1].astype(F32) for u in range(units)])
        summed = lax.psum_scatter(
            summed.reshape(units, rest, groups, blk, width),
            "dp",
            scatter_dimension=1,
            axis_index_groups=[[r * groups + g for r in range(rest)] for g in range(groups)],
            tiled=True,
        ).reshape(units, groups, blk, width)
        parts = [summed[u] for u in range(units)]
    pieces = call(
        functools.partial(sum_kernel, groups, units),
        [shape((units, blk, width), F32 if d == 0 else BF16) for d in range(groups)],
        *parts,
    )
    moved = [pieces[0]]
    for d in range(1, groups):
        moved.append(swap(pieces[d], "dp", ndp, d))
    pieces = moved
    pieces = [p.astype(F32) for p in pieces]
    stacked = jnp.stack(pieces).reshape(groups, per, halves, blk, width)
    order = jnp.stack([lax.dynamic_index_in_dim(stacked, mine ^ d, 0, False) for d in range(groups)])
    sub_key_grad = jnp.transpose(order, (3, 0, 1, 2, 4)).reshape(blk, heads, halves, width)

    rows = query_weight.shape[0]
    here = tok // ntensor
    early = [0] if groups > 1 else []
    late = list(range(len(early), groups))
    span = per * halves * width
    if early:
        begun = call(
            functools.partial(first_kernel, groups, early, per),
            shape((rows, tok), F32),
            *[qgs[d] for d in early],
            query_weight,
            scratch=[pltpu.VMEM((len(early) * span, tok), BF16)],
        )
    else:
        begun = jnp.zeros((rows, tok), F32)
    outs = call(
        functools.partial(second_kernel, groups, late, ntensor, per),
        [shape((rows, here), F32 if e == 0 else BF16) for e in range(ntensor)],
        *[qgs[d] for d in late],
        query_weight,
        begun,
        scratch=[pltpu.VMEM((len(late) * span, tok), BF16)],
    )
    outs = [outs[0]] + [swap(outs[e], "tensor", ntensor, e) for e in range(1, ntensor)]
    input_grad = call(join_kernel, shape((here, rows), BF16), *outs)
    return sub_key_grad, input_grad


def solution(mesh):
    in_specs = (
        P(("dp", "key"), "tensor", None, None),
        P("key", "tensor", None, None),
        P(None, "tensor"),
        P(("dp", "key"), "tensor", None, None),
        P(("dp", "key"), "tensor", None),
        P(("dp", "key"), "tensor", None),
        P(("dp", "key"), "tensor", None),
    )
    out_specs = (P(("dp", "key"), "tensor", None, None), P(("dp", "key", "tensor"), None))

    return jax.shard_map(
        on_device, mesh=mesh, in_specs=in_specs, out_specs=out_specs, check_vma=False
    )
```
